256 devices in a mesh: dp: 64 (over y, z, core), mp: 4 (over x).
Axes of the slice: x: 4, y: 4, z: 8, core: 2. Of those that a mesh axis runs over, the one named last changes fastest.
Arguments:
- queries: bfloat16 [32768, 4096], P('dp', 'mp'), may hold values from -6 to 6
- passages: bfloat16 [32768, 4096], P('dp', 'mp'), may hold values from -6 to 6
- labels: int32 [32768], P('dp'), may hold values from 0 to 32767
- projection: bfloat16 [4096, 128], P('mp'), may hold values from -0.09375 to 0.09375
Outputs:
- loss: float32 [32768], P('dp')
- query_embed: bfloat16 [32768, 128], P('dp')
The draws below stay inside these ranges and needn't reach their ends.
All inputs are finite; a program needn't handle non-finite values.
Results may differ from the reference program's by a relative error of at most 0.0039.
Values may be sent and summed in bfloat16 or wider, within the bound.
A program may use at most 64 MiB of HBM per device.

```python
import jax
import jax.numpy as jnp
from jax import lax

D = 4096
E = 128
BATCH = 32768


def draw_states(key, salt):
    subkey = jax.random.fold_in(key, salt)
    values = jnp.clip(jax.random.normal(subkey, (BATCH, D), jnp.float32), -6.0, 6.0)
    return values


def draw_passages(key, part):
    return draw_states(key, 11).astype(jnp.bfloat16)


def draw_queries(key, part):
    values = draw_states(key, 7)
    return values.astype(jnp.bfloat16)


def set_ends(values, key, smallest, largest):
    spot = [jax.random.randint(jax.random.fold_in(key, axis), (), 0, length) for axis, length in enumerate(values.shape)]
    main_axis = values.shape.index(max(values.shape))
    neighbour = spot[:main_axis] + [(spot[main_axis] + 1) % values.shape[main_axis]] + spot[main_axis + 1:]
    return values.at[tuple(spot)].set(smallest).at[tuple(neighbour)].set(largest)


def block_levels(own_key, dims, split, smallest, high):
    factor_of, own = 1.0, jax.random.fold_in(own_key, 6)
    for position, blocks in split:
        heights = jnp.exp(jax.random.uniform(jax.random.fold_in(own, position), (blocks,), jnp.float32, smallest / len(split), high / len(split)))
        factor_of = factor_of * jnp.repeat(heights, dims[position] // blocks).reshape([-1 if axis == position else 1 for axis in range(len(dims))])
    return factor_of


def normal_values(stream_key, extent, width, reach, shards=(), kind=jnp.bfloat16):
    drawn = jax.random.normal(stream_key, extent, jnp.float32) * width
    if len(shards) > 0:
        drawn = block_levels(stream_key, extent, shards, -0.22, 0.18) * drawn
    return jnp.clip(drawn, min=-reach, max=reach).astype(kind)


def setup_inputs(seed: int = 0) -> dict:
    keys = jax.random.split(jax.random.key(seed), 5)
    queries = draw_queries(jax.random.fold_in(keys[4], 71), 0)
    passages = draw_passages(jax.random.fold_in(keys[4], 71), 0)
    labels = set_ends(jax.random.randint(keys[2], (BATCH,), 0, BATCH), jax.random.fold_in(keys[2], 1), 0, BATCH - 1).astype(jnp.int32)
    projection = normal_values(keys[3], (D, E), D ** -0.5, 0.09375, ((0, 4),))
    return {"queries": queries, "passages": passages, "labels": labels, "projection": projection}


def reference(queries, passages, labels, projection):
    query_embed = jnp.dot(queries, projection, preferred_element_type=jnp.float32).astype(jnp.bfloat16)
    passage_embed = jnp.dot(passages, projection, preferred_element_type=jnp.float32).astype(jnp.bfloat16)
    block = min(512, BATCH)
    count = BATCH // block
    query_blocks = query_embed.reshape(count, block, E)
    label_blocks = labels.reshape(count, block)

    def one_block(args):
        qblock, lblock = args
        scores = jnp.dot(qblock, passage_embed.T, preferred_element_type=jnp.float32)
        total = jax.nn.logsumexp(scores, axis=1)
        chosen = jnp.take_along_axis(scores, lblock[:, None].astype(jnp.int32), axis=1)[:, 0]
        return total - chosen

    loss = lax.map(one_block, (query_blocks, label_blocks)).reshape(BATCH)
    return loss, query_embed
```

```python
import functools

import jax
import jax.numpy as jnp
from jax import lax
from jax.experimental import pallas as pl
from jax.experimental.pallas import tpu as pltpu
from jax.sharding import PartitionSpec as P

MESH = pl.DeviceIdType.MESH
X, Y, Z = 4, 4, 8
F32 = jnp.float32
BF16 = jnp.bfloat16


def signed_step(slot):
    return ((slot + 1) // 2) * (2 * (slot % 2) - 1)


def slot_of(step, size):
    if step == 0:
        return 0
    return 2 * step - 1 if step <= size // 2 else 2 * (size - step)


def kernel(
    queries,
    passages,
    labels,
    projection,
    loss_out,
    embed_out,
    weights,
    raw,
    part_send,
    part_recv,
    pas,
    qry,
    lab,
    target,
    top,
    total,
    chosen,
    stat_send,
    stat_recv,
    load_sem,
    store_sem,
    rs_send,
    rs_recv,
    lab_send,
    lab_recv,
    pz_send,
    pz_recv,
    pc_send,
    pc_recv,
    qa_send,
    qa_recv,
    qb_send,
    qb_recv,
    st_send,
    st_recv,
):
    dp = lax.axis_index("dp")
    x = lax.axis_index("mp")
    c = dp % 2
    z = (dp // 2) % Z
    y = dp // (2 * Z)
    share = raw.shape[2]

    def at(dx=0, dy=0, dz=0, other=False):
        core = 1 - c if other else c
        return ((((y + dy) % Y) * Z + (z + dz) % Z) * 2 + core, (x + dx) % X)

    def remote(src, dst, send, recv, device):
        return pltpu.make_async_remote_copy(
            src_ref=src,
            dst_ref=dst,
            send_sem=send,
            recv_sem=recv,
            device_id=device,
            device_id_type=MESH,
        )

    started = []

    def send(*args):
        copy = remote(*args)
        copy.start()
        started.append(copy)

    def arrived(dst, recv):
        remote(dst, dst, recv, recv, at(dx=1)).wait_recv()

    loads = {}
    first = pltpu.make_async_copy(projection, weights, load_sem.at[0])
    first.start()
    order = (2, 1, 3, 0)
    for tower, states in enumerate((passages, queries)):
        for r in order:
            rows = pl.ds(((x + r) % X) * share, share)
            copy = pltpu.make_async_copy(
                states.at[rows], raw.at[tower, r], load_sem.at[1 + tower * X + r]
            )
            copy.start()
            loads[tower, r] = copy

    peers = [at(dx=dx, dy=dy) for dx in range(X) for dy in range(Y) if dx or dy]
    peers += [at(dz=dz) for dz in range(1, Z)] + [at(other=True)]
    barrier = pltpu.get_barrier_semaphore()
    for peer in peers:
        pl.semaphore_signal(barrier, inc=1, device_id=peer, device_id_type=MESH)

    first.wait()

    def partial(tower, r):
        loads[tower, r].wait()
        return jnp.dot(raw[tower, r], weights[...], preferred_element_type=F32)

    for tower in range(2):
        for r in order[:-1]:
            part_send[tower, r] = partial(tower, r).astype(BF16)
        if tower == 0:
            pl.semaphore_wait(barrier, len(peers))
        for r in order[:-1]:
            send(
                part_send.at[tower, r],
                part_recv.at[tower, r],
                rs_send.at[tower, r],
                rs_recv.at[tower, r],
                at(dx=r),
            )
    for r in range(1, Y):
        send(labels, lab.at[slot_of(r, Y)], lab_send.at[r], lab_recv.at[r], at(dy=r))
    lab[0] = labels[...]
    own = [partial(tower, 0) for tower in range(2)]

    def summed(tower):
        value = own[tower]
        for r in (1, 3, 2):
            arrived(part_recv.at[tower, r], rs_recv.at[tower, r])
            value = value + part_recv[tower, r].astype(F32)
        return value.astype(BF16)

    pas[0, c] = summed(0)
    for r in (4, 3, 5, 2, 6, 1, 7):
        send(
            pas.at[0, c], pas.at[slot_of(r, Z), c], pz_send.at[r], pz_recv.at[r], at(dz=r)
        )
    send(pas.at[0, c], pas.at[0, c], pc_send.at[0], pc_recv.at[0], at(other=True))

    half = share // 2
    qry[0, x] = summed(1)

    def lines(slot, block, side):
        return qry.at[slot, block, pl.ds(side * half, half)]

    def forward_y(rx):
        block = (x - rx + X) % X
        for ry in (2, 1, 3):
            send(
                lines(0, block, 0),
                lines(slot_of(ry, Y), block, 0),
                qb_send.at[0, rx, ry],
                qb_recv.at[0, rx, ry],
                at(dy=ry),
            )

    def forward_x(ry):
        slot = slot_of(ry, Y)
        for rx in (2, 1, 3):
            send(
                lines(slot, x, 1),
                lines(slot, x, 1),
                qb_send.at[1, ry, rx],
                qb_recv.at[1, ry, rx],
                at(dx=rx),
            )

    for r in (2, 1, 3):
        send(lines(0, x, 0), lines(0, x, 0), qa_send.at[0, r], qa_recv.at[0, r], at(dx=r))
        send(
            lines(0, x, 1),
            lines(slot_of(r, Y), x, 1),
            qa_send.at[1, r],
            qa_recv.at[1, r],
            at(dy=r),
        )
    forward_y(0)
    forward_x(0)

    def relay_query(r):
        arrived(lines(0, (x - r + X) % X, 0), qa_recv.at[0, r])
        forward_y(r)
        arrived(lines(slot_of(r, Y), x, 1), qa_recv.at[1, r])
        forward_x(r)

    def relay_passage(r):
        slot = slot_of(r, Z)
        arrived(pas.at[slot, c], pz_recv.at[r])
        send(pas.at[slot, c], pas.at[slot, c], pc_send.at[r], pc_recv.at[r], at(other=True))

    def passage_here(r):
        arrived(pas.at[slot_of(r, Z), 1 - c], pc_recv.at[r])

    def queries_here(ry):
        slot = slot_of(ry, Y)
        for rx in range(X):
            block = (x - rx + X) % X
            if ry:
                arrived(lines(slot, block, 0), qb_recv.at[0, rx, ry])
            if rx:
                arrived(lines(slot, block, 1), qb_recv.at[1, ry, rx])
        if ry:
            arrived(lab.at[slot], lab_recv.at[ry])
        sub = lax.broadcasted_iota(jnp.int32, (8, share), 0)
        for block in range(X):
            where = pl.ds(block * share, share)
            line = lab[slot, pl.ds(block, 1), :]
            target[slot, :, where] = line - (y * Z * 2 * X + x) * share - sub
        top[slot] = jnp.full(top.shape[1:], -jnp.inf, F32)
        total[slot] = jnp.zeros(total.shape[1:], F32)
        chosen[slot] = jnp.zeros(chosen.shape[1:], F32)

    width = 2 * share

    def tile(group, slot):
        source = (z - signed_step(slot) + Z) % Z
        rows = pas[slot].reshape(2 * share, share)
        for part in range(X * share // width):
            cols = pl.ds(part * width, width)
            block = qry[group, pl.ds(2 * part, 2)].reshape(width, share)
            scores = lax.dot_general(
                rows, block, (((1,), (1,)), ((), ())), preferred_element_type=F32
            )
            aim = target[group, :, cols] - source * (2 * X * share)
            pick = chosen[group, :, cols]
            high = top[group, :, cols]
            before = high
            for k in range(2 * share // 8):
                line = scores[8 * k : 8 * k + 8]
                index = (8 * k // share) * X * share + 8 * k % share
                pick = jnp.where(aim == index, line, pick)
                high = jnp.maximum(high, line)
            chosen[group, :, cols] = pick
            top[group, :, cols] = high
            mass = total[group, :, cols] * jnp.exp(before - high)
            for k in range(2 * share // 8):
                mass = mass + jnp.exp(scores[8 * k : 8 * k + 8] - high)
            total[group, :, cols] = mass

    def tiles(group, low, high):
        def body(slot, carry):
            tile(group, slot)
            return carry

        lax.fori_loop(low, high, body, 0)

    def finish(group, ry):
        peak = jnp.max(top[group], axis=0, keepdims=True)
        mass = jnp.sum(total[group] * jnp.exp(top[group] - peak), axis=0, keepdims=True)
        lse = peak + jnp.log(mass)
        hit = jnp.sum(chosen[group], axis=0, keepdims=True)
        into = stat_recv if group == 0 else stat_send
        for place in (stat_send, stat_recv) if group == 0 else (stat_send,):
            for block in range(X):
                cut = slice(block * share, (block + 1) * share)
                place[group, pl.ds(block, 1), :] = lse[:, cut]
                place[group, pl.ds(X + block, 1), :] = hit[:, cut]
        for rx in (2, 1, 3, 0):
            if rx or ry:
                send(
                    stat_send.at[group],
                    stat_recv.at[rx * Y + group],
                    st_send.at[rx, group],
                    st_recv.at[rx, group],
                    at(dx=rx, dy=(Y - ry) % Y),
                )

    relay_query(1)
    relay_query(3)
    relay_passage(1)
    relay_passage(7)
    relay_query(2)
    relay_passage(2)
    relay_passage(6)
    passage_here(0)
    passage_here(1)
    passage_here(7)
    queries_here(0)
    stores = []
    for block in range(X):
        copy = pltpu.make_async_copy(
            qry.at[0, block], embed_out.at[pl.ds(block * share, share)], store_sem.at[block]
        )
        copy.start()
        stores.append(copy)
    tiles(0, 0, 3)
    relay_passage(3)
    relay_passage(5)
    passage_here(2)
    passage_here(6)
    tiles(0, 3, 5)
    queries_here(1)
    tiles(1, 0, 5)
    relay_passage(4)
    queries_here(3)
    tiles(2, 0, 5)
    passage_here(3)
    passage_here(5)
    for group in range(3):
        tiles(group, 5, 7)
    queries_here(2)
    passage_here(4)
    tiles(3, 0, 8)
    finish(3, 2)
    tiles(1, 7, 8)
    finish(1, 1)
    tiles(2, 7, 8)
    finish(2, 3)
    tiles(0, 7, 8)
    finish(0, 0)

    for rx in range(X):
        for group in range(Y):
            if rx or group:
                arrived(stat_recv.at[rx * Y + group], st_recv.at[rx, group])
    parts = stat_recv[...]
    lse, hit = parts[:, :X], parts[:, X:]
    peak = jnp.max(lse, axis=0)
    mass = jnp.sum(jnp.exp(lse - peak[None]), axis=0)
    loss_out[...] = peak + jnp.log(mass) - jnp.sum(hit, axis=0)

    for copy in stores:
        copy.wait()
    for copy in started:
        copy.wait_send()


def per_device(queries, passages, labels, projection):
    rows, depth = queries.shape
    embed = projection.shape[1]
    share = rows // X
    dma = pltpu.SemaphoreType.DMA
    vmem = pl.BlockSpec(memory_space=pltpu.VMEM)
    hbm = pl.BlockSpec(memory_space=pl.ANY)
    loss, query_embed = pl.pallas_call(
        kernel,
        out_shape=(
            jax.ShapeDtypeStruct((X, share), F32),
            jax.ShapeDtypeStruct((rows, embed), BF16),
        ),
        in_specs=[hbm, hbm, vmem, hbm],
        out_specs=(vmem, hbm),
        scratch_shapes=[
            pltpu.VMEM((depth, embed), BF16),
            pltpu.VMEM((2, X, share, depth), BF16),
            pltpu.VMEM((2, X, share, embed), BF16),
            pltpu.VMEM((2, X, share, embed), BF16),
            pltpu.VMEM((Z, 2, share, embed), BF16),
            pltpu.VMEM((Y, X, share, embed), BF16),
            pltpu.VMEM((Y, X, share), jnp.int32),
            pltpu.VMEM((Y, 8, rows), jnp.int32),
            pltpu.VMEM((Y, 8, rows), F32),
            pltpu.VMEM((Y, 8, rows), F32),
            pltpu.VMEM((Y, 8, rows), F32),
            pltpu.VMEM((Y, 2 * X, share), F32),
            pltpu.VMEM((X * Y, 2 * X, share), F32),
            dma((1 + 2 * X,)),
            dma((X,)),
            dma((2, X)),
            dma((2, X)),
            dma((Y,)),
            dma((Y,)),
            dma((Z,)),
            dma((Z,)),
            dma((Z,)),
            dma((Z,)),
            dma((2, X)),
            dma((2, X)),
            dma((2, X, Y)),
            dma((2, X, Y)),
            dma((X, Y)),
            dma((X, Y)),
        ],
        compiler_params=pltpu.CompilerParams(
            collective_id=0, has_side_effects=True, vmem_limit_bytes=67_000_000
        ),
    )(queries, passages, labels.reshape(X, share), projection)
    return loss.reshape(rows), query_embed


def solution(mesh):
    return jax.shard_map(
        per_device,
        mesh=mesh,
        in_specs=(P("dp", "mp"), P("dp", "mp"), P("dp"), P("mp", None)),
        out_specs=(P("dp"), P("dp", None)),
        check_vma=False,
    )
```
